32 devices in a mesh: groups: 2 (over y), feat: 4 (over x, core), loop: 4 (over z).
Axes of the slice: x: 2, y: 2, z: 4, core: 2. Of those that a mesh axis runs over, the one named last changes fastest.
Arguments:
- train_grads: bfloat16 [512, 65536], P(('groups', 'loop'), 'feat'), parts along dimension 0, may hold values from -6 to 6
- query_grads: bfloat16 [64, 65536], P(('groups', 'loop'), 'feat'), parts along dimension 0, may hold values from -0.0234375 to 0.0234375
- curvature: float32 [65536], P('feat'), may hold values from 0.05 to 5
- row_counts: int32 [8], P(('groups', 'loop')), parts along dimension 0, may hold values from 1 to 64, 128 in all
Outputs:
- scores: float32 [512, 32], P(('groups', 'loop', 'feat')), parts along dimension 0
The draws below stay inside these ranges and needn't reach their ends.
There are 2 independent parts, one for each index of `groups`. The reference program is written for one: setup_inputs(seed, part) draws one part's arguments, and reference() takes and returns one part's arrays. A program takes and returns all parts, laid end to end along the dimension named above; an argument that names none is the same for every part. Nothing has to cross between parts.
Inputs may be any that keep to these rules, and one draw needn't show every extreme that they name: row_counts[s] is the number of live slots of loop shard s; slots 0 to row_counts[s] - 1 of that shard are live; some shard has exactly 64; the counts sum to 128.
All inputs are finite; a program needn't handle non-finite values.
Results may differ from the reference program's by a relative error of at most 0.0029.
Values may be sent and summed in bfloat16 or wider, within the bound.
No kernel may reach another device: no remote copies, remote signals or barrier semaphores. Data moves between devices by JAX's collectives and lax.ppermute only.
A program may use at most 128 MiB of HBM per device.

```python
import math
import jax
import jax.numpy as jnp
import numpy as np

F = 65536
CAP = 64
TRAIN = 256
QUERIES = 32
N_LOOP = 4


def level_of(key, shape, split, low, top_value):
    loudness, own = 1.0, jax.random.fold_in(key, 6)
    for axis_at, parts in split:
        draws = jnp.exp(jax.random.uniform(jax.random.fold_in(own, axis_at), (parts,), jnp.float32, low / len(split), top_value / len(split)))
        loudness = loudness * jnp.repeat(draws, shape[axis_at] // parts).reshape([-1 if axis == axis_at else 1 for axis in range(len(shape))])
    return loudness


def profile(number_of, total, reach, lean):
    weights = [(1 << 20) // math.isqrt(grade ** lean) + 1 for grade in range(2, number_of + 1)]
    rest, counts = total - reach - (number_of - 1), [1] * (number_of - 1)
    while rest > 0:
        movable = [i for i in range(number_of - 1) if counts[i] < reach]
        mass, left = sum([weights[i] for i in movable]), rest
        for i in movable:
            addition = min(reach - counts[i], max(1, left * weights[i] // mass), rest)
            counts[i] = counts[i] + addition
            rest = rest - addition
    return np.array([reach] + counts)


def ragged_sizes(stream_key, count, total, reach, lean):
    if count == 2:
        one = jax.random.randint(stream_key, (), max(1, total - reach), min(reach, total - 1) + 1)
        return jnp.stack([one, total - one])
    tallies = jnp.asarray(profile(count, total, reach, lean), jnp.int32)
    pairs = (count - 1) // 2
    giver, receiver = tallies[1:1 + 2 * pairs:2], tallies[2:2 + 2 * pairs:2]
    room = jnp.minimum(giver - 1, reach - receiver)
    shifted = jax.random.randint(jax.random.fold_in(stream_key, 1), (pairs,), 0, 1 << 20) % (room + 1)
    tallies = tallies.at[1:1 + 2 * pairs:2].set(giver - shifted).at[2:2 + 2 * pairs:2].set(receiver + shifted)
    return tallies[jax.random.permutation(jax.random.fold_in(stream_key, 2), count)]


def bell_draw(own_key, dims, spread, bound, shards=(), kind=jnp.bfloat16):
    drawn = jax.random.normal(own_key, dims, jnp.float32) * spread
    if len(shards) > 0:
        drawn = level_of(own_key, dims, shards, -0.22, 0.18) * drawn
    return jnp.clip(drawn, min=-bound, max=bound).astype(kind)


def setup_inputs(seed: int = 0, part: int = 0) -> dict:
    key_of = jax.random.split(jax.random.key(seed), 5)
    part_keys = jax.random.split(jax.random.fold_in(key_of[4], part), 5)
    return {
        "train_grads": bell_draw(part_keys[0], (TRAIN, F), 1.0, 6.0, ((0, 4), (1, 4))),
        "query_grads": bell_draw(part_keys[1], (QUERIES, F), F ** -0.5, 0.0234375, ((0, 4), (1, 4))),
        "curvature": jnp.clip(jnp.exp(math.log(5.0) - 4.6051702 * jax.random.uniform(key_of[2], (F,), jnp.float32) ** level_of(key_of[2], (F,), ((0, 4),), -0.2, 0.2)), 0.05, 5.0),
        "row_counts": ragged_sizes(part_keys[3], N_LOOP, N_LOOP * CAP // 2, CAP, 2).astype(jnp.int32),
    }


damping_term = 0.1


def reference(train_grads, query_grads, curvature, row_counts):
    precond = (query_grads.astype(jnp.float32) / (damping_term + curvature[None, :])).astype(jnp.bfloat16)
    slots = jnp.arange(TRAIN, dtype=jnp.int32)
    shard_of = (slots // CAP).astype(jnp.int32)
    live = (slots % CAP) < row_counts[shard_of]
    raw = jnp.dot(train_grads, precond.T, preferred_element_type=jnp.float32)
    return jnp.where(live[:, None], raw, jnp.float32(0.0))
```

```python
import functools

import jax
import jax.numpy as jnp
from jax import lax
from jax.experimental import pallas as pl
from jax.experimental.pallas import tpu as pltpu
from jax.sharding import PartitionSpec as P

damping_term = 0.1


def scale_rows(block, curvature):
    return (block.astype(jnp.float32) / (damping_term + curvature)).astype(jnp.bfloat16)


def product(rows, piece):
    return lax.dot_general(
        rows, piece, (((1,), (1,)), ((), ())), preferred_element_type=jnp.float32
    )


def gathered(train_grads, query_grads, curvature, row_counts):
    slots = train_grads.shape[0]
    live = (jnp.arange(slots, dtype=jnp.int32) < row_counts[0])[:, None]
    queries = lax.all_gather(query_grads, "loop", axis=0, tiled=True)
    raw = product(train_grads, scale_rows(queries, curvature[None, :]))
    partial_scores = jnp.where(live, raw, jnp.float32(0.0))
    return lax.psum_scatter(partial_scores, "feat", scatter_dimension=0, tiled=True)


def score_kernel(shards, where_ref, count_ref, train_ref, curve_ref, *refs):
    pieces, outs, acc_t, acc = refs[: shards + 2], refs[shards + 2 : -2], refs[-2], refs[-1]
    me, part = where_ref[0], where_ref[1]
    damp = damping_term + curve_ref[...]
    train = train_ref[...]
    for hop in range(shards):
        rows = pieces[hop][...].astype(jnp.float32)
        if hop >= 2:
            rows = rows + pieces[hop + 2][...].astype(jnp.float32)
        scaled = (rows / damp).astype(jnp.bfloat16)
        acc_t[me ^ hop] = product(scaled, train)
    slots = train_ref.shape[0]
    table = acc_t[...].reshape(-1, slots).T
    live = lax.broadcasted_iota(jnp.int32, table.shape, 0) < count_ref[0]
    acc[...] = jnp.where(live, table, 0.0)
    height = outs[0].shape[0]
    for hop, out in enumerate(outs):
        out[...] = acc[pl.ds(pl.multiple_of((part ^ hop) * height, height), height), :]


def permuted(n_feat, train_grads, query_grads, curvature, row_counts):
    swap = lambda pairs: lax.ppermute(query_grads, "loop", pairs)
    far_in = swap([(0, 2), (3, 1)])
    near = swap([(0, 1), (1, 0), (2, 3), (3, 2)])
    far_out = swap([(1, 3), (2, 0)])
    middle = swap([(1, 2), (2, 1)])
    passed = lax.ppermute(far_in, "loop", [(2, 3), (1, 0)])
    me, part = lax.axis_index("loop"), lax.axis_index("feat")
    pieces = (query_grads, near, far_in, middle, far_out, passed)
    slots, features = train_grads.shape
    rows = query_grads.shape[0]
    queries = 4 * rows
    vmem = pl.BlockSpec(memory_space=pltpu.VMEM)
    smem = pl.BlockSpec(memory_space=pltpu.SMEM)
    block = jax.ShapeDtypeStruct((slots // n_feat, queries), jnp.float32)
    blocks = pl.pallas_call(
        functools.partial(score_kernel, 4),
        out_shape=[block] * n_feat,
        in_specs=[smem, smem] + [vmem] * (2 + len(pieces)),
        out_specs=[vmem] * n_feat,
        scratch_shapes=[
            pltpu.VMEM((4, rows, slots), jnp.float32),
            pltpu.VMEM((slots, queries), jnp.float32),
        ],
        compiler_params=pltpu.CompilerParams(vmem_limit_bytes=16 << 20),
        name="score",
    )(jnp.stack([me, part]), row_counts, train_grads, curvature[None, :], *pieces)
    total = blocks[0]
    for hop in range(1, n_feat):
        total = total + lax.ppermute(blocks[hop], "feat", [(i, i ^ hop) for i in range(n_feat)])
    return total


def solution(mesh):
    placed = (
        P(("groups", "loop"), "feat"),
        P(("groups", "loop"), "feat"),
        P("feat"),
        P(("groups", "loop")),
    )
    n_loop, n_feat = mesh.shape["loop"], mesh.shape["feat"]
    body = functools.partial(permuted, n_feat) if n_loop == 4 and n_feat & (n_feat - 1) == 0 else gathered
    return jax.shard_map(
        body,
        mesh=mesh,
        in_specs=placed,
        out_specs=P(("groups", "loop", "feat"), None),
        check_vma=False,
    )
```

```python
import functools

import jax
import jax.numpy as jnp
from jax import lax
from jax.experimental import pallas as pl
from jax.experimental.pallas import tpu as pltpu
from jax.sharding import PartitionSpec as P

damping_term = 0.1
vmem = pl.BlockSpec(memory_space=pltpu.VMEM)
smem = pl.BlockSpec(memory_space=pltpu.SMEM)
grant = pltpu.CompilerParams(vmem_limit_bytes=16 << 20)


def product(rows, piece):
    return lax.dot_general(
        rows, piece, (((1,), (1,)), ((), ())), preferred_element_type=jnp.float32
    )


def gathered(train_grads, query_grads, curvature, row_counts):
    slots = train_grads.shape[0]
    live = (jnp.arange(slots, dtype=jnp.int32) < row_counts[0])[:, None]
    queries = lax.all_gather(query_grads, "loop", axis=0, tiled=True).astype(jnp.float32)
    scaled = (queries / (damping_term + curvature[None, :])).astype(jnp.bfloat16)
    partial_scores = jnp.where(live, product(train_grads, scaled), jnp.float32(0.0))
    return lax.psum_scatter(partial_scores, "feat", scatter_dimension=0, tiled=True)


def own_kernel(train_ref, curve_ref, own_ref, score_ref, gain_ref):
    gain_ref[...] = 1.0 / (damping_term + curve_ref[...])
    own = own_ref[...]
    scaled = (own.astype(jnp.float32) * gain_ref[...]).astype(jnp.bfloat16)
    score_ref[...] = product(scaled, train_ref[...])


def early_kernel(train_ref, gain_ref, near_ref, far_ref, near_score, far_score):
    gain = gain_ref[...]
    near = near_ref[...].astype(jnp.float32) * gain
    near_score[...] = product(near.astype(jnp.bfloat16), train_ref[...])
    far = far_ref[...].astype(jnp.float32) * gain
    far_score[...] = product(far.astype(jnp.bfloat16), train_ref[...])


def last_kernel(where_ref, count_ref, train_ref, gain_ref, own, near, far, cross, *refs):
    outs, table, scores = refs[:-2], refs[-2], refs[-1]
    me, part = where_ref[0], where_ref[1]
    last = cross[...].astype(jnp.float32) * gain_ref[...]
    table[me] = own[...]
    table[me ^ 1] = near[...]
    table[me ^ 2] = far[...]
    table[me ^ 3] = product(last.astype(jnp.bfloat16), train_ref[...])
    slots = train_ref.shape[0]
    whole = table[...].reshape(-1, slots).T
    live = lax.broadcasted_iota(jnp.int32, whole.shape, 0) < count_ref[0]
    scores[...] = jnp.where(live, whole, 0.0)
    height = outs[0].shape[0]
    for hop, out in enumerate(outs):
        out[...] = scores[pl.ds(pl.multiple_of((part ^ hop) * height, height), height), :]


def permuted(n_feat, train_grads, query_grads, curvature, row_counts):
    slots, features = train_grads.shape
    rows = query_grads.shape[0]
    def send(piece, pairs):
        return lax.ppermute(piece, "loop", pairs)
    score = jax.ShapeDtypeStruct((rows, slots), jnp.float32)
    far = send(query_grads, [(i, i ^ 2) for i in range(4)])
    near = send(query_grads, [(i, i ^ 1) for i in range(4)])
    own_score, gain = pl.pallas_call(
        own_kernel,
        out_shape=[score, jax.ShapeDtypeStruct((1, features), jnp.float32)],
        in_specs=[vmem] * 3,
        out_specs=[vmem] * 2,
        compiler_params=grant,
        name="own",
    )(train_grads, curvature[None, :], query_grads)
    cross = send(far, [(i, i ^ 1) for i in range(4)])
    near_score, far_score = pl.pallas_call(
        early_kernel,
        out_shape=[score] * 2,
        in_specs=[vmem] * 4,
        out_specs=[vmem] * 2,
        compiler_params=grant,
        name="early",
    )(train_grads, gain, near, far)
    place = jnp.stack([lax.axis_index("loop"), lax.axis_index("feat")])
    block = jax.ShapeDtypeStruct((slots // n_feat, 4 * rows), jnp.float32)
    blocks = pl.pallas_call(
        last_kernel,
        out_shape=[block] * n_feat,
        in_specs=[smem] * 2 + [vmem] * 6,
        out_specs=[vmem] * n_feat,
        scratch_shapes=[
            pltpu.VMEM((4, rows, slots), jnp.float32),
            pltpu.VMEM((slots, 4 * rows), jnp.float32),
        ],
        compiler_params=grant,
        name="last",
    )(place, row_counts, train_grads, gain, own_score, near_score, far_score, cross)
    total = blocks[0]
    for hop in range(1, n_feat):
        total = total + lax.ppermute(blocks[hop], "feat", [(i, i ^ hop) for i in range(n_feat)])
    return total


def solution(mesh):
    placed = (
        P(("groups", "loop"), "feat"),
        P(("groups", "loop"), "feat"),
        P("feat"),
        P(("groups", "loop")),
    )
    n_loop, n_feat = mesh.shape["loop"], mesh.shape["feat"]
    short = n_loop == 4 and n_feat & (n_feat - 1) == 0
    return jax.shard_map(
        functools.partial(permuted, n_feat) if short else gathered,
        mesh=mesh,
        in_specs=placed,
        out_specs=P(("groups", "loop", "feat"), None),
        check_vma=False,
    )
```

```python
import functools

import jax
import jax.numpy as jnp
from jax import lax
from jax.experimental import pallas as pl
from jax.experimental.pallas import tpu as pltpu
from jax.sharding import PartitionSpec as P

damping_term = 0.1
vmem = pl.BlockSpec(memory_space=pltpu.VMEM)
smem = pl.BlockSpec(memory_space=pltpu.SMEM)
grant = pltpu.CompilerParams(vmem_limit_bytes=16 << 20)


def product(rows, piece):
    return lax.dot_general(
        rows, piece, (((1,), (1,)), ((), ())), preferred_element_type=jnp.float32
    )


def gathered(train_grads, query_grads, curvature, row_counts):
    slots = train_grads.shape[0]
    live = (jnp.arange(slots, dtype=jnp.int32) < row_counts[0])[:, None]
    queries = lax.all_gather(query_grads, "loop", axis=0, tiled=True).astype(jnp.float32)
    scaled = (queries / (damping_term + curvature[None, :])).astype(jnp.bfloat16)
    partial_scores = jnp.where(live, product(train_grads, scaled), jnp.float32(0.0))
    return lax.psum_scatter(partial_scores, "feat", scatter_dimension=0, tiled=True)


def scored(piece_ref, gain_ref, train_ref, start=0):
    span = pl.ds(start, piece_ref.shape[1])
    scaled = (piece_ref[...].astype(jnp.float32) * gain_ref[:, span]).astype(jnp.bfloat16)
    return product(scaled, train_ref[:, span])


def own_kernel(train_ref, curve_ref, own_ref, score_ref, gain_ref):
    gain_ref[...] = 1.0 / (damping_term + curve_ref[...])
    score_ref[...] = scored(own_ref, gain_ref, train_ref)


def early_kernel(train_ref, gain_ref, near, *refs):
    fars, near_score, far_score = refs[:-2], refs[-2], refs[-1]
    near_score[...] = scored(near, gain_ref, train_ref)
    start, total = 0, 0.0
    for far in fars:
        total = total + scored(far, gain_ref, train_ref, start)
        start += far.shape[1]
    far_score[...] = total


def mid_kernel(train_ref, gain_ref, *refs):
    start, total = 0, 0.0
    for cross in refs[:-1]:
        total = total + scored(cross, gain_ref, train_ref, start)
        start += cross.shape[1]
    refs[-1][...] = total


def last_kernel(count_ref, train_ref, gain_ref, own, near, far, cross, final, *refs):
    outs, table, scores = refs[:-2], refs[-2], refs[-1]
    me, part = lax.axis_index("loop"), lax.axis_index("feat")
    slots, features = train_ref.shape
    table[me] = own[...]
    table[me ^ 1] = near[...]
    table[me ^ 2] = far[...]
    table[me ^ 3] = cross[...] + scored(final, gain_ref, train_ref, features - final.shape[1])
    whole = table[...].reshape(-1, slots).T
    live = lax.broadcasted_iota(jnp.int32, whole.shape, 0) < count_ref[0]
    scores[...] = jnp.where(live, whole, 0.0)
    height = outs[0].shape[0]
    for hop, out in enumerate(outs):
        out[...] = scores[pl.ds(pl.multiple_of((part ^ hop) * height, height), height), :]


shares = (3, 3, 2)


def permuted(n_feat, train_grads, query_grads, curvature, row_counts):
    slots, features = train_grads.shape
    rows = query_grads.shape[0]

    def swap(piece, axis, mask):
        pairs = [(i, i ^ mask) for i in range(lax.axis_size(axis))]
        return lax.ppermute(piece, axis, pairs)

    def kernel(body, shapes, operands, smems=0, scratch=()):
        return pl.pallas_call(
            body,
            out_shape=shapes,
            in_specs=[smem] * smems + [vmem] * (len(operands) - smems),
            out_specs=[vmem] * len(shapes),
            scratch_shapes=scratch,
            compiler_params=grant,
        )(*operands)

    score = jax.ShapeDtypeStruct((rows, slots), jnp.float32)
    near = swap(query_grads, "loop", 1)
    ends = [features * sum(shares[: k + 1]) // sum(shares) for k in range(len(shares))]
    chunks, after = [], query_grads
    for start, end in zip([0] + ends, ends):
        chunks.append(after[:, start:end])
        after, _ = lax.optimization_barrier((after, chunks[-1]))
    far = [swap(chunk, "loop", 2) for chunk in chunks]
    own_score, gain = kernel(
        own_kernel,
        [score, jax.ShapeDtypeStruct((1, features), jnp.float32)],
        (train_grads, curvature[None, :], query_grads),
    )
    cross = [swap(piece, "loop", 1) for piece in far]
    near_score, far_score = kernel(early_kernel, [score] * 2, (train_grads, gain, near, *far))
    (cross_score,) = kernel(mid_kernel, [score], (train_grads, gain, *cross[:-1]))
    block = jax.ShapeDtypeStruct((slots // n_feat, 4 * rows), jnp.float32)
    blocks = kernel(
        last_kernel,
        [block] * n_feat,
        (row_counts, train_grads, gain, own_score, near_score, far_score, cross_score, cross[-1]),
        smems=1,
        scratch=[
            pltpu.VMEM((4, rows, slots), jnp.float32),
            pltpu.VMEM((slots, 4 * rows), jnp.float32),
        ],
    )
    total = blocks[0]
    for hop in range(1, n_feat):
        total = total + swap(blocks[hop], "feat", hop)
    return total


def solution(mesh):
    placed = (
        P(("groups", "loop"), "feat"),
        P(("groups", "loop"), "feat"),
        P("feat"),
        P(("groups", "loop")),
    )
    n_loop, n_feat = mesh.shape["loop"], mesh.shape["feat"]
    short = n_loop == 4 and n_feat & (n_feat - 1) == 0
    return jax.shard_map(
        functools.partial(permuted, n_feat) if short else gathered,
        mesh=mesh,
        in_specs=placed,
        out_specs=P(("groups", "loop", "feat"), None),
        check_vma=False,
    )
```

```python
import functools

import jax
import jax.numpy as jnp
from jax import lax
from jax.experimental import pallas as pl
from jax.experimental.pallas import tpu as pltpu
from jax.sharding import PartitionSpec as P

damping_term = 0.1
vmem = pl.BlockSpec(memory_space=pltpu.VMEM)
smem = pl.BlockSpec(memory_space=pltpu.SMEM)
grant = pltpu.CompilerParams(vmem_limit_bytes=16 << 20)


def product(rows, piece):
    return lax.dot_general(
        rows, piece, (((1,), (1,)), ((), ())), preferred_element_type=jnp.float32
    )


def gathered(train_grads, query_grads, curvature, row_counts):
    slots = train_grads.shape[0]
    live = (jnp.arange(slots, dtype=jnp.int32) < row_counts[0])[:, None]
    queries = lax.all_gather(query_grads, "loop", axis=0, tiled=True).astype(jnp.float32)
    scaled = (queries / (damping_term + curvature[None, :])).astype(jnp.bfloat16)
    partial_scores = jnp.where(live, product(train_grads, scaled), jnp.float32(0.0))
    return lax.psum_scatter(partial_scores, "feat", scatter_dimension=0, tiled=True)


def scored(piece_ref, gain_ref, train_ref, start=0):
    span = pl.ds(start, piece_ref.shape[1])
    scaled = (piece_ref[...].astype(jnp.float32) * gain_ref[:, span]).astype(jnp.bfloat16)
    return product(scaled, train_ref[:, span])


def own_kernel(train_ref, curve_ref, *refs):
    pieces, score_ref, gain_ref = refs[:-2], refs[-2], refs[-1]
    gain_ref[...] = 1.0 / (damping_term + curve_ref[...])
    start, total = 0, 0.0
    for piece in pieces:
        total = total + scored(piece, gain_ref, train_ref, start)
        start += piece.shape[1]
    score_ref[...] = total


def early_kernel(train_ref, gain_ref, *refs):
    pieces, sums = refs[:-2], refs[-2:]
    half = len(pieces) // 2
    for group, out in zip((pieces[:half], pieces[half:]), sums):
        start, total = 0, 0.0
        for piece in group:
            total = total + scored(piece, gain_ref, train_ref, start)
            start += piece.shape[1]
        out[...] = total


def mid_kernel(train_ref, gain_ref, *refs):
    start, total = 0, 0.0
    for cross in refs[:-1]:
        total = total + scored(cross, gain_ref, train_ref, start)
        start += cross.shape[1]
    refs[-1][...] = total


def last_kernel(count_ref, train_ref, gain_ref, own, near, far, cross, final, *refs):
    outs, table, scores = refs[:-2], refs[-2], refs[-1]
    me, part = lax.axis_index("loop"), lax.axis_index("feat")
    slots, features = train_ref.shape
    table[me] = own[...]
    table[me ^ 1] = near[...]
    table[me ^ 2] = far[...]
    table[me ^ 3] = cross[...] + scored(final, gain_ref, train_ref, features - final.shape[1])
    whole = table[...].reshape(-1, slots).T
    live = lax.broadcasted_iota(jnp.int32, whole.shape, 0) < count_ref[0]
    scores[...] = jnp.where(live, whole, 0.0)
    height = outs[0].shape[0]
    for hop, out in enumerate(outs):
        out[...] = scores[pl.ds(pl.multiple_of((part ^ hop) * height, height), height), :]


shares = (1, 1)


def permuted(n_feat, train_grads, query_grads, curvature, row_counts):
    slots, features = train_grads.shape
    rows = query_grads.shape[0]

    def swap(piece, axis, mask):
        pairs = [(i, i ^ mask) for i in range(lax.axis_size(axis))]
        return lax.ppermute(piece, axis, pairs)

    def kernel(body, shapes, operands, smems=0, scratch=()):
        return pl.pallas_call(
            body,
            out_shape=shapes,
            in_specs=[smem] * smems + [vmem] * (len(operands) - smems),
            out_specs=[vmem] * len(shapes),
            scratch_shapes=scratch,
            compiler_params=grant,
        )(*operands)

    score = jax.ShapeDtypeStruct((rows, slots), jnp.float32)
    ends = [features * sum(shares[: k + 1]) // sum(shares) for k in range(len(shares))]
    chunks, after = [], query_grads
    for start, end in zip([0] + ends, ends):
        chunks.append(after[:, start:end])
        after, _ = lax.optimization_barrier((after, chunks[-1]))
    n_loop = lax.axis_size("loop")

    def turns(piece, even, odd):
        pairs = [
            (part * n_loop + i, part * n_loop + (i ^ (odd if part & 1 else even)))
            for part in range(n_feat)
            for i in range(n_loop)
        ]
        return lax.ppermute(piece, ("feat", "loop"), pairs)

    odd = lax.axis_index("feat") & 1 == 1
    first = turns(chunks[0], 1, 2)
    second = turns(chunks[0], 2, 1)
    pick = lambda on_odd, on_even: jnp.where(odd, on_odd, on_even)
    far0, near0 = pick(first, second), pick(second, first)
    far = [far0] + [swap(chunk, "loop", 2) for k, chunk in enumerate(chunks) if k]
    near = [near0] + [swap(chunk, "loop", 1) for k, chunk in enumerate(chunks) if k]
    own_score, gain = kernel(
        own_kernel,
        [score, jax.ShapeDtypeStruct((1, features), jnp.float32)],
        (train_grads, curvature[None, :], *chunks),
    )
    cross = [swap(piece, "loop", 1) for piece in far]
    near_score, far_score = kernel(early_kernel, [score] * 2, (train_grads, gain, *near, *far))
    (cross_score,) = kernel(mid_kernel, [score], (train_grads, gain, *cross[:-1]))
    block = jax.ShapeDtypeStruct((slots // n_feat, 4 * rows), jnp.float32)
    blocks = kernel(
        last_kernel,
        [block] * n_feat,
        (row_counts, train_grads, gain, own_score, near_score, far_score, cross_score, cross[-1]),
        smems=1,
        scratch=[
            pltpu.VMEM((4, rows, slots), jnp.float32),
            pltpu.VMEM((slots, 4 * rows), jnp.float32),
        ],
    )
    total = blocks[0]
    for hop in range(1, n_feat):
        total = total + swap(blocks[hop], "feat", hop)
    return total


def solution(mesh):
    placed = (
        P(("groups", "loop"), "feat"),
        P(("groups", "loop"), "feat"),
        P("feat"),
        P(("groups", "loop")),
    )
    n_loop, n_feat = mesh.shape["loop"], mesh.shape["feat"]
    short = n_loop == 4 and n_feat & (n_feat - 1) == 0
    return jax.shard_map(
        functools.partial(permuted, n_feat) if short else gathered,
        mesh=mesh,
        in_specs=placed,
        out_specs=P(("groups", "loop", "feat"), None),
        check_vma=False,
    )
```

```python
import functools

import jax
import jax.numpy as jnp
from jax import lax
from jax.experimental import pallas as pl
from jax.experimental.pallas import tpu as pltpu
from jax.sharding import PartitionSpec as P

damping_term = 0.1
vmem = pl.BlockSpec(memory_space=pltpu.VMEM)
smem = pl.BlockSpec(memory_space=pltpu.SMEM)
grant = pltpu.CompilerParams(vmem_limit_bytes=16 << 20)


def product(rows, piece):
    return lax.dot_general(
        rows, piece, (((1,), (1,)), ((), ())), preferred_element_type=jnp.float32
    )


def gathered(train_grads, query_grads, curvature, row_counts):
    slots = train_grads.shape[0]
    live = (jnp.arange(slots, dtype=jnp.int32) < row_counts[0])[:, None]
    queries = lax.all_gather(query_grads, "loop", axis=0, tiled=True).astype(jnp.float32)
    scaled = (queries / (damping_term + curvature[None, :])).astype(jnp.bfloat16)
    partial_scores = jnp.where(live, product(train_grads, scaled), jnp.float32(0.0))
    return lax.psum_scatter(partial_scores, "feat", scatter_dimension=0, tiled=True)


def scored(piece_ref, gain_ref, train_ref, start=0):
    span = pl.ds(start, piece_ref.shape[1])
    scaled = (piece_ref[...].astype(jnp.float32) * gain_ref[:, span]).astype(jnp.bfloat16)
    return product(scaled, train_ref[:, span])


def own_kernel(train_ref, curve_ref, *refs):
    pieces, score_ref, gain_ref = refs[:-2], refs[-2], refs[-1]
    gain_ref[...] = 1.0 / (damping_term + curve_ref[...])
    start, total = 0, 0.0
    for piece in pieces:
        total = total + scored(piece, gain_ref, train_ref, start)
        start += piece.shape[1]
    score_ref[...] = total


def early_kernel(train_ref, gain_ref, *refs):
    pieces, sums = refs[:-2], refs[-2:]
    half = len(pieces) // 2
    for group, out in zip((pieces[:half], pieces[half:]), sums):
        start, total = 0, 0.0
        for piece in group:
            total = total + scored(piece, gain_ref, train_ref, start)
            start += piece.shape[1]
        out[...] = total


def mid_kernel(train_ref, gain_ref, *refs):
    start, total = 0, 0.0
    for cross in refs[:-1]:
        total = total + scored(cross, gain_ref, train_ref, start)
        start += cross.shape[1]
    refs[-1][...] = total


def last_kernel(count_ref, train_ref, gain_ref, own, near, far, cross, final, *refs):
    outs, table, scores = refs[:-2], refs[-2], refs[-1]
    me, part = lax.axis_index("loop"), lax.axis_index("feat")
    slots, features = train_ref.shape
    table[me] = own[...]
    table[me ^ 1] = near[...]
    table[me ^ 2] = far[...]
    table[me ^ 3] = cross[...] + scored(final, gain_ref, train_ref, features - final.shape[1])
    whole = table[...].reshape(-1, slots).T
    live = lax.broadcasted_iota(jnp.int32, whole.shape, 0) < count_ref[0]
    scores[...] = jnp.where(live, whole, 0.0)
    height = outs[0].shape[0]
    for hop, out in enumerate(outs):
        out[...] = scores[pl.ds(pl.multiple_of((part ^ hop) * height, height), height), :]


shares = (1, 1)


def permuted(n_feat, train_grads, query_grads, curvature, row_counts):
    slots, features = train_grads.shape
    rows = query_grads.shape[0]

    def swap(piece, axis, mask):
        pairs = [(i, i ^ mask) for i in range(lax.axis_size(axis))]
        return lax.ppermute(piece, axis, pairs)

    def kernel(body, shapes, operands, smems=0, scratch=()):
        return pl.pallas_call(
            body,
            out_shape=shapes,
            in_specs=[smem] * smems + [vmem] * (len(operands) - smems),
            out_specs=[vmem] * len(shapes),
            scratch_shapes=scratch,
            compiler_params=grant,
        )(*operands)

    score = jax.ShapeDtypeStruct((rows, slots), jnp.float32)
    ends = [features * sum(shares[: k + 1]) // sum(shares) for k in range(len(shares))]
    chunks, after = [], query_grads
    for start, end in zip([0] + ends, ends):
        chunks.append(after[:, start:end])
        after, _ = lax.optimization_barrier((after, chunks[-1]))
    n_loop = lax.axis_size("loop")

    def turns(piece, even, odd):
        pairs = [
            (part * n_loop + i, part * n_loop + (i ^ (odd if part & 1 else even)))
            for part in range(n_feat)
            for i in range(n_loop)
        ]
        return lax.ppermute(piece, ("feat", "loop"), pairs)

    odd = lax.axis_index("feat") & 1 == 1
    first = turns(chunks[0], 1, 2)
    second = turns(chunks[0], 2, 1)
    pick = lambda on_odd, on_even: jnp.where(odd, on_odd, on_even)
    far0, near0 = pick(first, second), pick(second, first)
    third = turns(chunks[1], 2, 1)
    fourth = turns(chunks[1], 1, 2)
    far1, near1 = pick(fourth, third), pick(third, fourth)
    far, near = [far0, far1], [near0, near1]
    own_score, gain = kernel(
        own_kernel,
        [score, jax.ShapeDtypeStruct((1, features), jnp.float32)],
        (train_grads, curvature[None, :], *chunks),
    )
    cross = [swap(piece, "loop", 1) for piece in far]
    near_score, far_score = kernel(early_kernel, [score] * 2, (train_grads, gain, *near, *far))
    (cross_score,) = kernel(mid_kernel, [score], (train_grads, gain, *cross[:-1]))
    block = jax.ShapeDtypeStruct((slots // n_feat, 4 * rows), jnp.float32)
    blocks = kernel(
        last_kernel,
        [block] * n_feat,
        (row_counts, train_grads, gain, own_score, near_score, far_score, cross_score, cross[-1]),
        smems=1,
        scratch=[
            pltpu.VMEM((4, rows, slots), jnp.float32),
            pltpu.VMEM((slots, 4 * rows), jnp.float32),
        ],
    )
    total = blocks[0]
    for hop in range(1, n_feat):
        total = total + swap(blocks[hop], "feat", hop)
    return total


def solution(mesh):
    placed = (
        P(("groups", "loop"), "feat"),
        P(("groups", "loop"), "feat"),
        P("feat"),
        P(("groups", "loop")),
    )
    n_loop, n_feat = mesh.shape["loop"], mesh.shape["feat"]
    short = n_loop == 4 and n_feat & (n_feat - 1) == 0
    return jax.shard_map(
        functools.partial(permuted, n_feat) if short else gathered,
        mesh=mesh,
        in_specs=placed,
        out_specs=P(("groups", "loop", "feat"), None),
        check_vma=False,
    )
```
